32 devices in a mesh: tm: 8 (over z, x), head: 4 (over y, core).
Axes of the slice: x: 2, y: 2, z: 4, core: 2. Of those that a mesh axis runs over, the one named last changes fastest.
Arguments:
- queries: bfloat16 [18432, 1024], P(('tm', 'head')), may hold values from -8 to 8
- keys: bfloat16 [18432, 1024], P(('tm', 'head')), may hold values from -8 to 8
- values: bfloat16 [18432, 1024], P(('tm', 'head')), may hold values from -6 to 6
- tile_list: int32 [48, 7], P('tm'), may hold values from 0 to 47, as said below
- tile_count: int32 [48], P('tm'), may hold values from 1 to 7
Outputs:
- attended: bfloat16 [18432, 1024], P(('tm', 'head'))
The draws below stay inside these ranges and needn't reach their ends.
Inputs may be any that keep to these rules, and one draw needn't show every extreme that they name: `tile_list`: row t lists distinct tiles of t's time slab (tiles t // 6 * 6 and on) and of the slabs just before and after it; the first slot is t itself; every slot holds such a tile, also past the count.
All inputs are finite; a program needn't handle non-finite values.
Results may differ from the reference program's by a relative error of at most 0.0046.
Values may be sent and summed in bfloat16 or wider, within the bound.
No kernel may reach another device: no remote copies, remote signals or barrier semaphores. Data moves between devices by JAX's collectives and lax.ppermute only.
A program may use at most 64 MiB of HBM per device.

```python
import jax
import jax.numpy as jnp
from jax import lax

HD = 128
TILE = 384
TILES_SLAB = 6
MAXLIST = 7
HEADS = 8
TOKENS = 18432
N_TM = 8


def draw_queries(key, part):
    drawn = jax.random.normal(jax.random.fold_in(key, 1), (TOKENS, HEADS * HD), jnp.float32)
    drawn = jnp.clip(drawn, -8.0, 8.0)
    return drawn.astype(jnp.bfloat16)


def draw_keys(key, part):
    drawn = jax.random.normal(jax.random.fold_in(key, 2), (TOKENS, HEADS * HD), jnp.float32)
    drawn = jnp.clip(drawn, -8.0, 8.0)
    return drawn.astype(jnp.bfloat16)


def tile_choice(key):
    all_tiles = TILES_SLAB * N_TM
    window_tiles = 3 * TILES_SLAB
    own_tile = jnp.arange(all_tiles, dtype=jnp.int32)
    slab_index = own_tile // TILES_SLAB
    offsets = jnp.arange(window_tiles, dtype=jnp.int32)
    candidates = (slab_index[:, None] - 1) * TILES_SLAB + offsets[None, :]
    usable = (candidates >= 0) & (candidates < all_tiles)
    rank_draw = jax.random.randint(jax.random.fold_in(key, 21), (all_tiles, window_tiles), 0, 1000)
    priority = rank_draw * window_tiles + offsets[None, :]
    priority = jnp.where(candidates == own_tile[:, None], 1001 * window_tiles, priority)
    priority = jnp.where(usable, priority, -1)
    unused, picked = lax.top_k(priority, MAXLIST)
    listed = jnp.take_along_axis(candidates, picked, axis=1).astype(jnp.int32)
    counts = jax.random.randint(jax.random.fold_in(key, 22), (all_tiles,), 1, MAXLIST + 1)
    at_edge = (slab_index == 0) | (slab_index == N_TM - 1)
    counts = jnp.where(at_edge, (counts + 1) // 2, counts)
    forced = jax.random.randint(jax.random.fold_in(key, 23), (), TILES_SLAB, all_tiles - TILES_SLAB)
    counts = jnp.where(own_tile == forced, MAXLIST, counts)
    return (listed, counts.astype(jnp.int32))


def draw_tile_list(key, part):
    return tile_choice(key)[0]


def draw_tile_count(key, part):
    return tile_choice(key)[1]


def steps_of(rng, dims, pieces, smallest, high):
    loudness = 1.0
    for dim, blocks in pieces:
        draws = jax.random.uniform(jax.random.fold_in(jax.random.fold_in(rng, 6), dim), (blocks,), jnp.float32, smallest / len(pieces), high / len(pieces))
        loudness = loudness * jnp.repeat(jnp.exp(draws), dims[dim] // blocks).reshape((-1,) + (1,) * (len(dims) - 1 - dim))
    return loudness


def gaussian(rng, shape, deviation, limit, pieces=(), held_as=jnp.bfloat16):
    values = deviation * jax.random.normal(rng, shape, jnp.float32)
    if pieces:
        values = values * steps_of(rng, shape, pieces, -0.22, 0.18)
    return jnp.clip(values, -limit, limit).astype(held_as)


def setup_inputs(seed: int = 0) -> dict:
    splits = jax.random.split(jax.random.key(seed), 6)
    queries = draw_queries(jax.random.fold_in(splits[5], 71), 0)
    keys = draw_keys(jax.random.fold_in(splits[5], 71), 0)
    values = gaussian(splits[2], (TOKENS, HEADS * HD), 1.0, 6.0, ((0, 32),))
    tile_list = draw_tile_list(jax.random.fold_in(splits[5], 71), 0)
    tile_count = draw_tile_count(jax.random.fold_in(splits[5], 71), 0)
    return {"queries": queries, "keys": keys, "values": values, "tile_list": tile_list, "tile_count": tile_count}


def reference(queries, keys, values, tile_list, tile_count):
    all_tiles = tile_list.shape[0]
    row_width = queries.shape[1]
    head_total = row_width // HD
    query_four = queries.reshape(all_tiles, TILE, head_total, HD)
    key_four = keys.reshape(all_tiles, TILE, head_total, HD)
    value_four = values.reshape(all_tiles, TILE, head_total, HD)
    key_span = MAXLIST * TILE
    slot_tile = jnp.arange(key_span, dtype=jnp.int32) // TILE
    scaling = HD ** -0.5

    def per_tile(operands):
        query_tile, listed, live_count = operands
        key_block = jnp.take(key_four, listed, axis=0).reshape(key_span, head_total, HD)
        value_block = jnp.take(value_four, listed, axis=0).reshape(key_span, head_total, HD)
        scores = jnp.einsum("qhd,khd->hqk", query_tile.astype(jnp.float32), key_block.astype(jnp.float32)) * scaling
        live_slots = slot_tile < live_count
        scores = jnp.where(live_slots[None, None, :], scores, -jnp.inf)
        highest = jnp.max(scores, axis=-1, keepdims=True)
        raised = jnp.exp(scores - highest)
        totals = jnp.sum(raised, axis=-1)
        weights = lax.optimization_barrier(raised.astype(jnp.bfloat16)).astype(jnp.float32)
        accumulated = jnp.einsum("hqk,khd->qhd", weights, value_block.astype(jnp.float32))
        return (accumulated / jnp.transpose(totals)[:, :, None]).astype(jnp.bfloat16)

    output = lax.map(per_tile, (query_four, tile_list, tile_count))
    return output.reshape(-1, row_width)
```

```python
import functools

import jax
import jax.numpy as jnp
import numpy as np
from jax import lax
from jax.experimental import pallas as pl
from jax.experimental.pallas import tpu as pltpu
from jax.sharding import Mesh, PartitionSpec as P

HD = 128
TILE = 384
LOG2E = 1.4426950408889634


def split_kernel(*refs):
    half = len(refs) // 2
    for source, target in zip(refs[:half], refs[half:]):
        target[0] = source[...]


def split_heads(arrays, pieces):
    tokens, row_width = arrays[0].shape
    width = row_width // pieces
    return pl.pallas_call(
        split_kernel,
        grid=(pieces,),
        in_specs=[pl.BlockSpec((tokens, width), lambda i: (0, i))] * len(arrays),
        out_specs=[pl.BlockSpec((1, tokens, width), lambda i: (i, 0, 0))] * len(arrays),
        out_shape=[jax.ShapeDtypeStruct((pieces, tokens, width), a.dtype) for a in arrays],
        name="split_heads",
    )(*arrays)


def join_kernel(source, target):
    target[...] = source[0]


def join_heads(array):
    pieces, tokens, width = array.shape
    return pl.pallas_call(
        join_kernel,
        grid=(pieces,),
        in_specs=[pl.BlockSpec((1, tokens, width), lambda i: (i, 0, 0))],
        out_specs=pl.BlockSpec((tokens, width), lambda i: (0, i)),
        out_shape=jax.ShapeDtypeStruct((tokens, pieces * width), array.dtype),
        name="join_heads",
    )(array)


def attend_kernel(
    list_ref,
    count_ref,
    q_ref,
    k_low,
    k_own,
    k_high,
    v_low,
    v_own,
    v_high,
    out_ref,
    k_all,
    v_all,
    s_even,
    s_odd,
    acc,
    stats,
):
    tiles = q_ref.shape[0]
    low = k_low.shape[0]
    own = k_own.shape[0]
    high = k_high.shape[0]
    factor = HD**-0.5 * LOG2E
    for parts, target in (((k_low, k_own, k_high), k_all), ((v_low, v_own, v_high), v_all)):
        target[0:low] = parts[0][...]
        target[low : low + own] = parts[1][...]
        target[low + own : low + own + high] = parts[2][...]
    acc[...] = jnp.zeros_like(acc)
    stats[...] = jnp.zeros_like(stats)

    def score(tile, slot, target):
        listed = list_ref[tile, slot]
        target[...] = lax.dot_general(
            k_all[listed],
            q_ref[tile],
            (((1,), (1,)), ((), ())),
            preferred_element_type=jnp.float32,
        )

    def following(tile, slot):
        more = slot + 1 < count_ref[tile]
        return jnp.where(more, tile, jnp.minimum(tile + 1, tiles - 1)), jnp.where(more, slot + 1, 0)

    def step(tile, slot, index, total, source, target):
        next_tile, next_slot = following(tile, slot)
        score(next_tile, next_slot, target)
        scores = source[...]
        before = jnp.where(slot == 0, -1e30, stats[0:1])
        highest = jnp.maximum(before, jnp.max(scores, axis=0, keepdims=True))
        raised = jnp.exp2((scores - highest) * factor)
        kept = jnp.exp2((before - highest) * factor)
        sums = stats[8:9] * kept + jnp.sum(raised, axis=0, keepdims=True)
        update = lax.dot_general(
            v_all[list_ref[tile, slot]],
            raised.astype(jnp.bfloat16),
            (((0,), (0,)), ((), ())),
            preferred_element_type=jnp.float32,
        )
        value = acc[...] * kept + update
        acc[...] = value
        stats[0:1] = highest
        stats[8:9] = sums

        @pl.when((slot + 1 == count_ref[tile]) & (index < total))
        def _():
            out_ref[tile] = jnp.transpose(value / sums).astype(out_ref.dtype)

        return next_tile, next_slot

    total = lax.fori_loop(0, tiles, lambda t, n: n + count_ref[t], jnp.int32(0))
    score(0, 0, s_even)

    def body(i, where):
        tile, slot = where
        tile, slot = step(tile, slot, 2 * i, total, s_even, s_odd)
        return step(tile, slot, 2 * i + 1, total, s_odd, s_even)

    lax.fori_loop(0, (total + 1) // 2, body, (jnp.int32(0), jnp.int32(0)))


def attend(q, k_parts, v_parts, listed, count):
    tiles = q.shape[0]
    window = sum(k.shape[0] for k in k_parts)
    vmem = pl.BlockSpec(memory_space=pltpu.VMEM)
    smem = pl.BlockSpec(memory_space=pltpu.SMEM)
    return pl.pallas_call(
        attend_kernel,
        in_specs=[smem, smem] + [vmem] * 7,
        out_specs=vmem,
        out_shape=jax.ShapeDtypeStruct(q.shape, q.dtype),
        scratch_shapes=[
            pltpu.VMEM((window, TILE, HD), q.dtype),
            pltpu.VMEM((window, TILE, HD), q.dtype),
            pltpu.VMEM((TILE, TILE), jnp.float32),
            pltpu.VMEM((TILE, TILE), jnp.float32),
            pltpu.VMEM((HD, TILE), jnp.float32),
            pltpu.VMEM((16, TILE), jnp.float32),
        ],
        cost_estimate=pl.CostEstimate(
            flops=4 * tiles * 4 * TILE * TILE * HD, bytes_accessed=8 * q.size, transcendentals=0
        ),
        name="attend",
    )(listed, count, q, *k_parts, *v_parts)


def shards(group_size, queries, keys, values, tile_list, tile_count):
    groups = lax.axis_size("group")
    head_size = lax.axis_size("head")
    members = group_size * head_size
    tokens, row_width = queries.shape
    width = row_width // members
    head_dev = width // HD
    slab_tiles = tile_list.shape[0]

    plan = jnp.concatenate([tile_list, tile_count[:, None]], axis=1)
    plan = lax.all_gather(plan, "member", axis=0, tiled=True)
    listed = plan[:, :-1] - (lax.axis_index("group") * group_size - 1) * slab_tiles
    count = plan[:, -1]

    def exchange(pieces):
        return lax.all_to_all(pieces, ("member", "head"), 0, 0, tiled=True)

    def halo(level):
        by_slab = level.reshape(group_size, head_size * tokens, width)
        up = [(i, i + 1) for i in range(groups - 1)]
        down = [(i + 1, i) for i in range(groups - 1)]
        low = lax.ppermute(by_slab[group_size - 1], "group", up)
        high = lax.ppermute(by_slab[0], "group", down)
        return low, level, high

    q_split, k_split, v_split = split_heads([queries, keys, values], members)
    k_parts = halo(exchange(k_split))
    v_parts = halo(exchange(v_split))
    q_level = exchange(q_split)

    def tiles_of(part, head):
        return part.reshape(-1, TILE, width)[:, :, head * HD : (head + 1) * HD]

    outputs = [
        attend(
            tiles_of(q_level, head),
            [tiles_of(part, head) for part in k_parts],
            [tiles_of(part, head) for part in v_parts],
            listed,
            count,
        )
        for head in range(head_dev)
    ]
    output = outputs[0] if head_dev == 1 else jnp.concatenate(outputs, axis=-1)
    return join_heads(exchange(output.reshape(members, tokens, width)))


def solution(mesh):
    tm_size, head_size = mesh.shape["tm"], mesh.shape["head"]

    def run(queries, keys, values, tile_list, tile_count):
        heads_dev = queries.shape[1] // HD // head_size
        group_size = heads_dev if tm_size % heads_dev == 0 else 1
        fine = Mesh(
            mesh.devices.reshape(tm_size // group_size, group_size, head_size),
            ("group", "member", "head"),
        )
        tokens_spec = P(("group", "member", "head"), None)
        return jax.shard_map(
            functools.partial(shards, group_size),
            mesh=fine,
            in_specs=(
                tokens_spec,
                tokens_spec,
                tokens_spec,
                P(("group", "member"), None),
                P(("group", "member")),
            ),
            out_specs=tokens_spec,
            check_vma=False,
        )(queries, keys, values, tile_list, tile_count)

    return run
```

```python
import functools

import jax
import jax.numpy as jnp
from jax import lax
from jax.experimental import pallas as pl
from jax.experimental.pallas import tpu as pltpu
from jax.sharding import Mesh, PartitionSpec as P


HD = 128
TILE = 384
UNROLL = 4
LOG2E = 1.4426950408889634
SPLIT_VMEM = 61 * 2**20
AXES = ("group", "member", "head")

ANY = pl.BlockSpec(memory_space=pl.ANY)
HBM = pl.BlockSpec(memory_space=pltpu.HBM)
SMEM = pl.BlockSpec(memory_space=pltpu.SMEM)
VMEM = pl.BlockSpec(memory_space=pltpu.VMEM)


def split_kernel_q(count, arrays, meta_ref, *refs):
    sources, targets = refs[:arrays], refs[arrays : arrays + count]
    stage, in_sems, out_sems = refs[arrays + count :]
    width = stage.shape[-1]

    def read(step, array):
        column = pl.multiple_of((meta_ref[0] ^ step) * width, width)
        return pltpu.make_async_copy(
            sources[array].at[:, pl.ds(column, width)], stage.at[step, array], in_sems.at[step, array]
        )

    def write(step):
        return pltpu.make_async_copy(stage.at[step], targets[step], out_sems.at[step])

    order = list(range(count - 1, -1, -1))
    for step in order:
        for array in range(arrays):
            read(step, array).start()
    for step in order:
        for array in range(arrays):
            read(step, array).wait()
        write(step).start()
    for step in order:
        write(step).wait()


def split_queries(meta, sources, count):
    tokens, row_width = sources[0].shape
    arrays = len(sources)
    piece = (arrays, tokens, row_width // count)
    return pl.pallas_call(
        functools.partial(split_kernel_q, count, arrays),
        in_specs=[SMEM] + [HBM] * arrays,
        out_specs=[ANY] * count,
        out_shape=[jax.ShapeDtypeStruct(piece, sources[0].dtype)] * count,
        scratch_shapes=[
            pltpu.VMEM((count,) + piece, sources[0].dtype),
            pltpu.SemaphoreType.DMA((count, arrays)),
            pltpu.SemaphoreType.DMA((count,)),
        ],
        compiler_params=pltpu.CompilerParams(vmem_limit_bytes=8 * 2**20),
        name="split_queries",
    )(meta, *sources)


def split_kernel(layout, meta_ref, *refs):
    sources, targets = refs[:2], refs[2 : 2 + len(layout)]
    stage, in_sems, out_sems = refs[2 + len(layout) :]
    width = stage.shape[-1]

    def read(slot, step, array):
        column = pl.multiple_of((meta_ref[0] ^ step) * width, width)
        return pltpu.make_async_copy(
            sources[array].at[:, pl.ds(column, width)], stage.at[slot, array], in_sems.at[slot, array]
        )

    reads, writes, slot = [], [], 0
    for index, steps in enumerate(layout):
        reads.append([read(slot + k, s, array) for k, s in enumerate(steps) for array in range(2)])
        block = stage.at[slot] if len(steps) == 1 else stage.at[pl.ds(slot, len(steps))]
        writes.append(pltpu.make_async_copy(block, targets[index], out_sems.at[index]))
        slot += len(steps)
    for copies in reads:
        for copy in copies:
            copy.start()
    for copies, write in zip(reads, writes):
        for copy in copies:
            copy.wait()
        write.start()
    for write in writes:
        write.wait()


def split_heads(meta, keys, values, layout, members):
    tokens, row_width = keys.shape
    piece = (2, tokens, row_width // members)
    shapes = [piece if len(steps) == 1 else (len(steps),) + piece for steps in layout]
    return pl.pallas_call(
        functools.partial(split_kernel, layout),
        in_specs=[SMEM] + [HBM] * 2,
        out_specs=[ANY] * len(layout),
        out_shape=[jax.ShapeDtypeStruct(shape, keys.dtype) for shape in shapes],
        scratch_shapes=[
            pltpu.VMEM((members,) + piece, keys.dtype),
            pltpu.SemaphoreType.DMA((members, 2)),
            pltpu.SemaphoreType.DMA((len(layout),)),
        ],
        compiler_params=pltpu.CompilerParams(vmem_limit_bytes=SPLIT_VMEM),
        name="split_heads",
    )(meta, keys, values)


def join_kernel(count, meta_ref, *refs):
    sources, target, sems = refs[:count], refs[count], refs[count + 1]
    width = sources[0].shape[-1]
    copies = []
    for step in range(count):
        column = pl.multiple_of((meta_ref[0] ^ step) * width, width)
        copies.append(
            pltpu.make_async_copy(sources[step], target.at[:, pl.ds(column, width)], sems.at[step])
        )
    for copy in copies:
        copy.start()
    for copy in copies:
        copy.wait()


def join_heads(meta, pieces):
    count = len(pieces)
    tokens, width = pieces[0].shape
    return pl.pallas_call(
        functools.partial(join_kernel, count),
        in_specs=[SMEM] + [VMEM] * count,
        out_specs=HBM,
        out_shape=jax.ShapeDtypeStruct((tokens, count * width), pieces[0].dtype),
        scratch_shapes=[pltpu.SemaphoreType.DMA((count,))],
        compiler_params=pltpu.CompilerParams(vmem_limit_bytes=4 * 2**20),
        name="join_heads",
    )(meta, *pieces)


def pack_kernel(first, second, target):
    target[0] = first[...]
    target[1] = second[...]


def pack(first, second):
    return pl.pallas_call(
        pack_kernel,
        in_specs=[VMEM] * 2,
        out_specs=VMEM,
        out_shape=jax.ShapeDtypeStruct((2,) + first.shape, first.dtype),
        compiler_params=pltpu.CompilerParams(vmem_limit_bytes=4 * 2**20),
        name="pack",
    )(first, second)


def assemble_kernel(places, members, head_size, meta_ref, *refs):
    arrays, targets = refs[:-2], refs[-2:]
    tokens = arrays[0].shape[-2]
    slab = head_size * tokens
    own = members * tokens
    for array, inner, step, halo in places:
        source = meta_ref[0] ^ step
        lane = (source % head_size) * tokens
        if halo:
            start = lane + jnp.where(source < head_size, slab + own, 0)
        else:
            start = slab + source * tokens
        rows = pl.ds(pl.multiple_of(start, 16), tokens)
        for part in range(2):
            ref = arrays[array]
            targets[part][rows] = ref[part] if inner is None else ref[inner, part]


def assemble(meta, pieces, members, head_size):
    arrays = [piece[0] for piece in pieces]
    places = [(i, inner, step, halo) for i, (_, inner, step, halo) in enumerate(pieces)]
    tokens, width = arrays[0].shape[-2:]
    window = (members + 2 * head_size) * tokens
    return pl.pallas_call(
        functools.partial(assemble_kernel, places, members, head_size),
        in_specs=[SMEM] + [VMEM] * len(arrays),
        out_specs=[VMEM] * 2,
        out_shape=[jax.ShapeDtypeStruct((window, width), arrays[0].dtype)] * 2,
        compiler_params=pltpu.CompilerParams(vmem_limit_bytes=24 * 2**20),
        name="assemble",
    )(meta, *arrays)


def fold(value, op):
    parts = [value[i * 8 : (i + 1) * 8] for i in range(value.shape[0] // 8)]
    while len(parts) > 1:
        rest = [parts[-1]] if len(parts) % 2 else []
        parts = [op(a, b) for a, b in zip(parts[::2], parts[1::2])] + rest
    return parts[0]


def rows_of(tile):
    return pl.ds(pl.multiple_of(tile * TILE, TILE), TILE)


def attend_kernel(parts, pieces, meta_ref, *refs):
    outputs = len(parts) * pieces
    plan_refs, q_refs = refs[: len(parts)], refs[len(parts) : len(parts) + outputs]
    keys, values = refs[len(parts) + outputs : len(parts) + outputs + 2]
    out_refs = refs[-9 - outputs : -9]
    item_tile, item_slot, item_key, q_part, out_part, raw, peaks, acc, totals = refs[-9:]
    tokens = q_refs[0].shape[0]
    block = pieces * tokens
    block_tiles = block // TILE
    tiles = len(parts) * block_tiles
    slab_tiles, slots = plan_refs[0].shape[0], plan_refs[0].shape[1] - 1
    me, base = meta_ref[0], meta_ref[1]
    factor = HD**-0.5 * LOG2E

    def piece_rows(index, step):
        row = index * block + ((me % pieces) ^ step) * tokens
        return pl.ds(pl.multiple_of(row, 16), tokens)

    for index in range(len(parts)):
        for step in range(pieces):
            q_part[piece_rows(index, step)] = q_refs[index * pieces + step][...]
    acc[...] = jnp.zeros_like(acc)
    totals[...] = jnp.zeros_like(totals)

    total = jnp.int32(0)
    for index, part in enumerate(parts):
        plan_ref = plan_refs[index]
        first_row = (((me // pieces) ^ part) * block_tiles) % slab_tiles
        for tile in range(block_tiles):
            for slot in range(slots):
                item_tile[total + slot] = jnp.int32(index * block_tiles + tile)
                item_slot[total + slot] = jnp.int32(slot)
                item_key[total + slot] = plan_ref[first_row + tile, slot] - base
            total = total + plan_ref[first_row + tile, slots]
    for extra in range(UNROLL):
        item_tile[total + extra] = jnp.int32(tiles)
        item_slot[total + extra] = jnp.int32(0)
        item_key[total + extra] = jnp.int32(0)

    def score(item, buffer):
        tile = jnp.minimum(item_tile[item], tiles - 1)
        scores = lax.dot_general(
            keys[rows_of(item_key[item])],
            q_part[rows_of(tile)],
            (((1,), (1,)), ((), ())),
            preferred_element_type=jnp.float32,
        )
        raw[buffer] = scores
        peaks[buffer] = fold(scores, jnp.maximum)

    def gather(item, buffer, highest, sums):
        tile = item_tile[item]
        before = jnp.where(item_slot[item] == 0, -1e30, highest)
        highest = jnp.maximum(before, jnp.max(peaks[buffer], axis=0, keepdims=True))
        kept = jnp.exp2((before - highest) * factor)
        raised = jnp.exp2((raw[buffer] - highest) * factor)
        sums = sums * kept + jnp.sum(fold(raised, jnp.add), axis=0, keepdims=True)
        update = lax.dot_general(
            values[rows_of(item_key[item])],
            raised.astype(jnp.bfloat16),
            (((0,), (0,)), ((), ())),
            preferred_element_type=jnp.float32,
        )
        acc[tile] = acc[tile] * kept + update
        totals[tile] = sums
        return highest, sums

    score(0, 0)

    def body(i, carry):
        for step in range(UNROLL):
            item = i * UNROLL + step
            score(item + 1, (step + 1) % 2)
            carry = gather(item, step % 2, *carry)
        return carry

    blank = jnp.zeros((1, TILE), jnp.float32)
    lax.fori_loop(0, (total + UNROLL - 1) // UNROLL, body, (blank, blank))
    for tile in range(tiles):
        out_part[tile * TILE : (tile + 1) * TILE] = jnp.transpose(acc[tile] / totals[tile]).astype(
            out_part.dtype
        )
    for index in range(len(parts)):
        for step in range(pieces):
            out_refs[index * pieces + step][...] = out_part[piece_rows(index, step)]


def attend(meta, plans, queries, keys, values, parts, pieces):
    tokens, width = queries[0].shape
    dtype = queries[0].dtype
    rows = len(parts) * pieces * tokens
    tiles = rows // TILE
    items = tiles * (plans[0].shape[1] - 1) + UNROLL + 8
    outputs = len(parts) * pieces
    return pl.pallas_call(
        functools.partial(attend_kernel, parts, pieces),
        in_specs=[SMEM] * (1 + len(parts)) + [VMEM] * (outputs + 2),
        out_specs=[VMEM] * outputs,
        out_shape=[jax.ShapeDtypeStruct((tokens, width), dtype)] * outputs,
        scratch_shapes=[pltpu.SMEM((items,), jnp.int32)] * 3
        + [pltpu.VMEM((rows, width), dtype)] * 2
        + [
            pltpu.VMEM((2, TILE, TILE), jnp.float32),
            pltpu.VMEM((2, 8, TILE), jnp.float32),
            pltpu.VMEM((tiles + 1, HD, TILE), jnp.float32),
            pltpu.VMEM((tiles + 1, 1, TILE), jnp.float32),
        ],
        compiler_params=pltpu.CompilerParams(vmem_limit_bytes=20 * 2**20),
        cost_estimate=pl.CostEstimate(
            flops=16 * rows * TILE * HD, bytes_accessed=4 * rows * width, transcendentals=0
        ),
        name="attend",
    )(meta, *plans, *queries, keys, values)


def pieces_of(tokens):
    pieces = 1
    while pieces * tokens % TILE:
        pieces *= 2
    return pieces


def shards(group_size, queries, keys, values, tile_list, tile_count):
    groups = lax.axis_size("group")
    head_size = lax.axis_size("head")
    members = group_size * head_size
    tokens = queries.shape[0]
    slab_tiles = tile_list.shape[0]
    pieces = pieces_of(tokens)
    meta = jnp.stack(
        [
            lax.axis_index("member") * head_size + lax.axis_index("head"),
            (lax.axis_index("group") * group_size - 1) * slab_tiles,
        ]
    ).astype(jnp.int32)

    def swap(piece, step):
        if step == 0:
            return piece
        pairs = [(g * members + i, g * members + (i ^ step)) for g in range(groups) for i in range(members)]
        return lax.ppermute(piece, AXES, pairs)

    def relay(piece, step):
        pairs = []
        for g in range(groups):
            for i in range(members):
                member = (i ^ step) // head_size
                if member == group_size - 1 and g + 1 < groups:
                    pairs.append((g * members + i, (g + 1) * members + i))
                if member == 0 and g > 0:
                    pairs.append((g * members + i, (g - 1) * members + i))
        return lax.ppermute(piece, AXES, pairs)

    own_plan = jnp.concatenate([tile_list, tile_count[:, None]], axis=1)
    plans = [swap(own_plan, step * head_size) for step in range(group_size)]

    layout = layout_of(members)
    kv_split = split_heads(meta, keys, values, layout, members)
    swapped = {s: swap(array, s) for (s,), array in zip(layout, kv_split)}
    pieces_kv = [(array, None, step, False) for step, array in swapped.items()]
    for step in range(members // 4, members):
        beyond = relay(swapped[step], step)
        pieces_kv.append((beyond, None, step, True))
    for step in range(0, members // 4, 2):
        pair = pack(swapped[step], swapped[step + 1])
        beyond = relay(pair, step)
        pieces_kv += [(beyond, inner, step + inner, True) for inner in range(2)]

    q_split = split_queries(meta, [queries], members)
    q_pieces = [swap(piece[0], step) for step, piece in enumerate(q_split)]
    window_keys, window_values = assemble(meta, pieces_kv, members, head_size)

    results = [None] * members
    for parts in calls_of(members // pieces):
        outputs = attend(
            meta,
            [plans[part * pieces // head_size] for part in parts],
            [q_pieces[part * pieces + step] for part in parts for step in range(pieces)],
            window_keys,
            window_values,
            parts,
            pieces,
        )
        steps = [part * pieces + step for part in parts for step in range(pieces)]
        for step, output in zip(steps, outputs):
            results[step] = swap(output, step)
    return join_heads(meta, results)


def calls_of(parts):
    return [(parts - 1,), tuple(range(parts - 2, 0, -1)), (0,)]


def layout_of(members):
    half = members // 2
    return [(s,) for s in [*range(members - 1, half - 1, -1), *range(half // 2, half), *range(half // 2)]]


def solution(mesh):
    tm_size, head_size = mesh.shape["tm"], mesh.shape["head"]

    def run(queries, keys, values, tile_list, tile_count):
        group_size = queries.shape[1] // HD // head_size
        members = group_size * head_size
        if group_size < 2 or tm_size % group_size or members & (members - 1):
            raise ValueError("unsupported mesh")
        fine = Mesh(mesh.devices.reshape(tm_size // group_size, group_size, head_size), AXES)
        tokens_spec = P(AXES, None)
        step = jax.shard_map(
            functools.partial(shards, group_size),
            mesh=fine,
            in_specs=(
                tokens_spec,
                tokens_spec,
                tokens_spec,
                P(("group", "member"), None),
                P(("group", "member")),
            ),
            out_specs=tokens_spec,
            check_vma=False,
        )
        return step(queries, keys, values, tile_list, tile_count)

    return run
```

```python
import functools

import jax
import jax.numpy as jnp
from jax import lax
from jax.experimental import pallas as pl
from jax.experimental.pallas import tpu as pltpu
from jax.sharding import Mesh, PartitionSpec as P


HD = 128
TILE = 384
UNROLL = 6
LOG2E = 1.4426950408889634
SPLIT_VMEM = 61 * 2**20
AXES = ("group", "member", "head")

ANY = pl.BlockSpec(memory_space=pl.ANY)
HBM = pl.BlockSpec(memory_space=pltpu.HBM)
SMEM = pl.BlockSpec(memory_space=pltpu.SMEM)
VMEM = pl.BlockSpec(memory_space=pltpu.VMEM)


def own_index():
    return lax.axis_index("member") * lax.axis_size("head") + lax.axis_index("head")


def split_kernel_q(members, source, *refs):
    pairs = members // 2
    targets = refs[:pairs]
    stage, in_sems, out_sems = refs[pairs:]
    width = stage.shape[-1]

    def read(step):
        column = pl.multiple_of((own_index() ^ step) * width, width)
        return pltpu.make_async_copy(
            source.at[:, pl.ds(column, width)], stage.at[step], in_sems.at[step]
        )

    def write(pair):
        return pltpu.make_async_copy(
            stage.at[pl.ds(2 * pair, 2)], targets[pair], out_sems.at[pair]
        )

    for step in range(members):
        read(step).start()
    for pair in range(pairs):
        read(2 * pair).wait()
        read(2 * pair + 1).wait()
        write(pair).start()
    for pair in range(pairs):
        write(pair).wait()


def split_queries(source, members):
    tokens, row_width = source.shape
    piece = (tokens, row_width // members)
    return pl.pallas_call(
        functools.partial(split_kernel_q, members),
        in_specs=[HBM],
        out_specs=[ANY] * (members // 2),
        out_shape=[jax.ShapeDtypeStruct((2,) + piece, source.dtype)] * (members // 2),
        scratch_shapes=[
            pltpu.VMEM((members,) + piece, source.dtype),
            pltpu.SemaphoreType.DMA((members,)),
            pltpu.SemaphoreType.DMA((members // 2,)),
        ],
        compiler_params=pltpu.CompilerParams(vmem_limit_bytes=8 * 2**20),
        name="split_queries",
    )(source)


def split_kernel(layout, *refs):
    sources, targets = refs[:2], refs[2 : 2 + len(layout)]
    stage, in_sems, out_sems = refs[2 + len(layout) :]
    width = stage.shape[-1]

    def read(slot, step, array):
        column = pl.multiple_of((own_index() ^ step) * width, width)
        return pltpu.make_async_copy(
            sources[array].at[:, pl.ds(column, width)], stage.at[slot, array], in_sems.at[slot, array]
        )

    reads, writes, slot = [], [], 0
    for index, steps in enumerate(layout):
        reads.append([read(slot + k, s, array) for k, s in enumerate(steps) for array in range(2)])
        block = stage.at[slot] if len(steps) == 1 else stage.at[pl.ds(slot, len(steps))]
        writes.append(pltpu.make_async_copy(block, targets[index], out_sems.at[index]))
        slot += len(steps)
    for copies in reads:
        for copy in copies:
            copy.start()
    for copies, write in zip(reads, writes):
        for copy in copies:
            copy.wait()
        write.start()
    for write in writes:
        write.wait()


def split_heads(keys, values, layout, members):
    tokens, row_width = keys.shape
    piece = (2, tokens, row_width // members)
    shapes = [piece if len(steps) == 1 else (len(steps),) + piece for steps in layout]
    return pl.pallas_call(
        functools.partial(split_kernel, layout),
        in_specs=[HBM] * 2,
        out_specs=[ANY] * len(layout),
        out_shape=[jax.ShapeDtypeStruct(shape, keys.dtype) for shape in shapes],
        scratch_shapes=[
            pltpu.VMEM((members,) + piece, keys.dtype),
            pltpu.SemaphoreType.DMA((members, 2)),
            pltpu.SemaphoreType.DMA((len(layout),)),
        ],
        compiler_params=pltpu.CompilerParams(vmem_limit_bytes=SPLIT_VMEM),
        name="split_heads",
    )(keys, values)


def join_kernel(count, *refs):
    sources, target, sems = refs[:count], refs[count], refs[count + 1]
    width = sources[0].shape[-1]
    copies = []
    for step in range(count):
        column = pl.multiple_of((own_index() ^ step) * width, width)
        copies.append(
            pltpu.make_async_copy(sources[step], target.at[:, pl.ds(column, width)], sems.at[step])
        )
    for copy in copies:
        copy.start()
    for copy in copies:
        copy.wait()


def join_heads(pieces):
    count = len(pieces)
    tokens, width = pieces[0].shape
    return pl.pallas_call(
        functools.partial(join_kernel, count),
        in_specs=[VMEM] * count,
        out_specs=HBM,
        out_shape=jax.ShapeDtypeStruct((tokens, count * width), pieces[0].dtype),
        scratch_shapes=[pltpu.SemaphoreType.DMA((count,))],
        compiler_params=pltpu.CompilerParams(vmem_limit_bytes=4 * 2**20),
        name="join_heads",
    )(*pieces)


def pack_kernel(first, second, target):
    target[0] = first[...]
    target[1] = second[...]


def pack(first, second):
    return pl.pallas_call(
        pack_kernel,
        in_specs=[VMEM] * 2,
        out_specs=VMEM,
        out_shape=jax.ShapeDtypeStruct((2,) + first.shape, first.dtype),
        compiler_params=pltpu.CompilerParams(vmem_limit_bytes=4 * 2**20),
        name="pack",
    )(first, second)


def assemble_kernel(places, members, head_size, *refs):
    arrays, targets = refs[:-2], refs[-2:]
    tokens = arrays[0].shape[-2]
    slab = head_size * tokens
    own = members * tokens
    for array, inner, step, halo in places:
        source = own_index() ^ step
        lane = (source % head_size) * tokens
        if halo:
            start = lane + jnp.where(source < head_size, slab + own, 0)
        else:
            start = slab + source * tokens
        rows = pl.ds(pl.multiple_of(start, 16), tokens)
        for part in range(2):
            ref = arrays[array]
            targets[part][rows] = ref[part] if inner is None else ref[inner, part]


def assemble(pieces, members, head_size):
    arrays = [piece[0] for piece in pieces]
    places = [(i, inner, step, halo) for i, (_, inner, step, halo) in enumerate(pieces)]
    tokens, width = arrays[0].shape[-2:]
    window = (members + 2 * head_size) * tokens
    return pl.pallas_call(
        functools.partial(assemble_kernel, places, members, head_size),
        in_specs=[VMEM] * len(arrays),
        out_specs=[VMEM] * 2,
        out_shape=[jax.ShapeDtypeStruct((window, width), arrays[0].dtype)] * 2,
        compiler_params=pltpu.CompilerParams(vmem_limit_bytes=24 * 2**20),
        name="assemble",
    )(*arrays)


def fold(value, op):
    parts = [value[i * 8 : (i + 1) * 8] for i in range(value.shape[0] // 8)]
    while len(parts) > 1:
        rest = [parts[-1]] if len(parts) % 2 else []
        parts = [op(a, b) for a, b in zip(parts[::2], parts[1::2])] + rest
    return parts[0]


def rows_of(tile):
    return pl.ds(pl.multiple_of(tile * TILE, TILE), TILE)


def attend_kernel(parts, pieces, *refs):
    outputs = len(parts) * pieces
    plan_in, q_refs = refs[: len(parts)], refs[len(parts) : len(parts) + outputs]
    keys, values = refs[len(parts) + outputs : len(parts) + outputs + 2]
    out_refs = refs[-11 - outputs : -11]
    plans, sems, item_tile, item_slot, item_key, q_part, out_part, raw, peaks, acc, totals = refs[-11:]
    tokens = q_refs[0].shape[1]
    block = pieces * tokens
    block_tiles = block // TILE
    tiles = len(parts) * block_tiles
    slab_tiles, slots = plan_in[0].shape[0], plan_in[0].shape[1] - 1
    copies = [
        pltpu.make_async_copy(plan, plans.at[i], sems.at[i]) for i, plan in enumerate(plan_in)
    ]
    for copy in copies:
        copy.start()
    me = own_index()
    base = (lax.axis_index("group") * lax.axis_size("member") - 1) * slab_tiles
    factor = HD**-0.5 * LOG2E

    def piece_rows(index, step):
        row = index * block + ((me % pieces) ^ step) * tokens
        return pl.ds(pl.multiple_of(row, 16), tokens)

    for index in range(len(parts)):
        for step in range(pieces):
            q_part[piece_rows(index, step)] = q_refs[index * pieces + step][step % 2]
    acc[...] = jnp.zeros_like(acc)
    totals[...] = jnp.zeros_like(totals)

    for copy in copies:
        copy.wait()
    total = jnp.int32(0)
    for index, part in enumerate(parts):
        first_row = (((me // pieces) ^ part) * block_tiles) % slab_tiles
        for tile in range(block_tiles):
            for slot in range(slots):
                item_tile[total + slot] = jnp.int32(index * block_tiles + tile)
                item_slot[total + slot] = jnp.int32(slot)
                item_key[total + slot] = plans[index, first_row + tile, slot] - base
            total = total + plans[index, first_row + tile, slots]
    for extra in range(UNROLL):
        item_tile[total + extra] = jnp.int32(tiles)
        item_slot[total + extra] = jnp.int32(0)
        item_key[total + extra] = jnp.int32(0)

    def score(item, buffer):
        tile = jnp.minimum(item_tile[item], tiles - 1)
        scores = lax.dot_general(
            keys[rows_of(item_key[item])],
            q_part[rows_of(tile)],
            (((1,), (1,)), ((), ())),
            preferred_element_type=jnp.float32,
        )
        raw[buffer] = scores
        peaks[buffer] = fold(scores, jnp.maximum)

    def gather(item, buffer, highest, sums):
        tile = item_tile[item]
        before = jnp.where(item_slot[item] == 0, -1e30, highest)
        highest = jnp.maximum(before, jnp.max(peaks[buffer], axis=0, keepdims=True))
        kept = jnp.exp2((before - highest) * factor)
        raised = jnp.exp2((raw[buffer] - highest) * factor)
        sums = sums * kept + jnp.sum(fold(raised, jnp.add), axis=0, keepdims=True)
        update = lax.dot_general(
            values[rows_of(item_key[item])],
            raised.astype(jnp.bfloat16),
            (((0,), (0,)), ((), ())),
            preferred_element_type=jnp.float32,
        )
        acc[tile] = acc[tile] * kept + update
        totals[tile] = sums
        return highest, sums

    score(0, 0)

    def chunk(size, start):
        def body(i, carry):
            for step in range(size):
                item = start + i * size + step
                score(item + 1, (step + 1) % 2)
                carry = gather(item, step % 2, *carry)
            return carry

        return body

    blank = jnp.zeros((1, TILE), jnp.float32)
    whole = total // UNROLL
    carry = lax.fori_loop(0, whole, chunk(UNROLL, 0), (blank, blank))
    rest = total - whole * UNROLL
    lax.fori_loop(0, (rest + 1) // 2, chunk(2, whole * UNROLL), carry)
    for tile in range(tiles):
        out_part[tile * TILE : (tile + 1) * TILE] = jnp.transpose(acc[tile] / totals[tile]).astype(
            out_part.dtype
        )
    for index in range(len(parts)):
        for step in range(pieces):
            out_refs[index * pieces + step][...] = out_part[piece_rows(index, step)]


def attend(plans, queries, keys, values, parts, pieces):
    _, tokens, width = queries[0].shape
    dtype = queries[0].dtype
    rows = len(parts) * pieces * tokens
    tiles = rows // TILE
    items = tiles * (plans[0].shape[1] - 1) + UNROLL + 8
    outputs = len(parts) * pieces
    return pl.pallas_call(
        functools.partial(attend_kernel, parts, pieces),
        in_specs=[VMEM] * (len(parts) + outputs + 2),
        out_specs=[VMEM] * outputs,
        out_shape=[jax.ShapeDtypeStruct((tokens, width), dtype)] * outputs,
        scratch_shapes=[
            pltpu.SMEM((len(parts),) + plans[0].shape, jnp.int32),
            pltpu.SemaphoreType.DMA((len(parts),)),
        ]
        + [pltpu.SMEM((items,), jnp.int32)] * 3
        + [pltpu.VMEM((rows, width), dtype)] * 2
        + [
            pltpu.VMEM((2, TILE, TILE), jnp.float32),
            pltpu.VMEM((2, 8, TILE), jnp.float32),
            pltpu.VMEM((tiles + 1, HD, TILE), jnp.float32),
            pltpu.VMEM((tiles + 1, 1, TILE), jnp.float32),
        ],
        compiler_params=pltpu.CompilerParams(vmem_limit_bytes=20 * 2**20),
        cost_estimate=pl.CostEstimate(
            flops=16 * rows * TILE * HD, bytes_accessed=4 * rows * width, transcendentals=0
        ),
        name="attend",
    )(*plans, *queries, keys, values)


def pieces_of(tokens):
    pieces = 1
    while pieces * tokens % TILE:
        pieces *= 2
    return pieces


def shards(group_size, queries, keys, values, tile_list, tile_count):
    groups = lax.axis_size("group")
    head_size = lax.axis_size("head")
    members = group_size * head_size
    tokens = queries.shape[0]
    pieces = pieces_of(tokens)

    def swap(piece, step):
        if step == 0:
            return piece
        pairs = [(g * members + i, g * members + (i ^ step)) for g in range(groups) for i in range(members)]
        return lax.ppermute(piece, AXES, pairs)

    def relay(piece, step):
        pairs = []
        for g in range(groups):
            for i in range(members):
                member = (i ^ step) // head_size
                if member == group_size - 1 and g + 1 < groups:
                    pairs.append((g * members + i, (g + 1) * members + i))
                if member == 0 and g > 0:
                    pairs.append((g * members + i, (g - 1) * members + i))
        return lax.ppermute(piece, AXES, pairs)

    own_plan = jnp.concatenate([tile_list, tile_count[:, None]], axis=1)
    plans = [swap(own_plan, step * head_size) for step in range(group_size)]

    layout = layout_of(members)
    kv_split = split_heads(keys, values, layout, members)
    swapped = {s: swap(array, s) for (s,), array in zip(layout, kv_split)}
    pieces_kv = [(array, None, step, False) for step, array in swapped.items()]
    for step in range(members // 4, members):
        beyond = relay(swapped[step], step)
        pieces_kv.append((beyond, None, step, True))
    for step in range(0, members // 4, 2):
        pair = pack(swapped[step], swapped[step + 1])
        beyond = relay(pair, step)
        pieces_kv += [(beyond, inner, step + inner, True) for inner in range(2)]

    q_split = split_queries(queries, members)
    q_pieces = []
    for pair, piece in enumerate(q_split):
        piece = swap(piece, 2 * pair)
        q_pieces += [piece, swap(piece, 1)]
    window_keys, window_values = assemble(pieces_kv, members, head_size)

    results = [None] * members
    for parts in calls_of(members // pieces):
        outputs = attend(
            [plans[part * pieces // head_size] for part in parts],
            [q_pieces[part * pieces + step] for part in parts for step in range(pieces)],
            window_keys,
            window_values,
            parts,
            pieces,
        )
        steps = [part * pieces + step for part in parts for step in range(pieces)]
        for step, output in zip(steps, outputs):
            results[step] = swap(output, step)
    return join_heads(results)


def calls_of(parts):
    return [(parts - 1,), tuple(range(parts - 2, 0, -1)), (0,)]


def layout_of(members):
    half = members // 2
    return [(s,) for s in [*range(members - 1, half - 1, -1), *range(half // 2, half), *range(half // 2)]]


def solution(mesh):
    tm_size, head_size = mesh.shape["tm"], mesh.shape["head"]

    def run(queries, keys, values, tile_list, tile_count):
        group_size = queries.shape[1] // HD // head_size
        members = group_size * head_size
        if group_size < 2 or members < 8 or tm_size % group_size or members & (members - 1):
            raise ValueError("unsupported mesh")
        fine = Mesh(mesh.devices.reshape(tm_size // group_size, group_size, head_size), AXES)
        tokens_spec = P(AXES, None)
        step = jax.shard_map(
            functools.partial(shards, group_size),
            mesh=fine,
            in_specs=(
                tokens_spec,
                tokens_spec,
                tokens_spec,
                P(("group", "member"), None),
                P(("group", "member")),
            ),
            out_specs=tokens_spec,
            check_vma=False,
        )
        return step(queries, keys, values, tile_list, tile_count)

    return run
```

```python
import functools

import jax
import jax.numpy as jnp
from jax import lax
from jax.experimental import pallas as pl
from jax.experimental.pallas import tpu as pltpu
from jax.sharding import Mesh, PartitionSpec as P


HD = 128
TILE = 384
UNROLL = 6
LOG2E = 1.4426950408889634
SPLIT_VMEM = 61 * 2**20
AXES = ("group", "member", "head")

ANY = pl.BlockSpec(memory_space=pl.ANY)
HBM = pl.BlockSpec(memory_space=pltpu.HBM)
SMEM = pl.BlockSpec(memory_space=pltpu.SMEM)
VMEM = pl.BlockSpec(memory_space=pltpu.VMEM)


def own_index():
    return lax.axis_index("member") * lax.axis_size("head") + lax.axis_index("head")


def split_kernel_q(layout, source, *refs):
    targets = refs[: len(layout)]
    stage, in_sems, out_sems = refs[len(layout) :]
    width = stage.shape[-1]

    def read(step):
        column = pl.multiple_of((own_index() ^ step) * width, width)
        return pltpu.make_async_copy(
            source.at[:, pl.ds(column, width)], stage.at[step], in_sems.at[step]
        )

    def write(index):
        first, size = layout[index][0], len(layout[index])
        block = stage.at[first] if size == 1 else stage.at[pl.ds(first, size)]
        return pltpu.make_async_copy(block, targets[index], out_sems.at[index])

    for steps in layout:
        for step in steps:
            read(step).start()
    for index, steps in enumerate(layout):
        for step in steps:
            read(step).wait()
        write(index).start()
    for index in range(len(layout)):
        write(index).wait()


def split_queries(source, layout, members):
    tokens, row_width = source.shape
    piece = (tokens, row_width // members)
    shapes = [piece if len(steps) == 1 else (len(steps),) + piece for steps in layout]
    return pl.pallas_call(
        functools.partial(split_kernel_q, layout),
        in_specs=[HBM],
        out_specs=[ANY] * len(layout),
        out_shape=[jax.ShapeDtypeStruct(shape, source.dtype) for shape in shapes],
        scratch_shapes=[
            pltpu.VMEM((members,) + piece, source.dtype),
            pltpu.SemaphoreType.DMA((members,)),
            pltpu.SemaphoreType.DMA((len(layout),)),
        ],
        compiler_params=pltpu.CompilerParams(vmem_limit_bytes=8 * 2**20),
        name="split_queries",
    )(source)


def split_kernel(layout, *refs):
    sources, targets = refs[:2], refs[2 : 2 + len(layout)]
    stage, in_sems, out_sems = refs[2 + len(layout) :]
    width = stage.shape[-1]

    def read(slot, step, array):
        column = pl.multiple_of((own_index() ^ step) * width, width)
        return pltpu.make_async_copy(
            sources[array].at[:, pl.ds(column, width)], stage.at[slot, array], in_sems.at[slot, array]
        )

    reads, writes, slot = [], [], 0
    for index, steps in enumerate(layout):
        reads.append([read(slot + k, s, array) for k, s in enumerate(steps) for array in range(2)])
        block = stage.at[slot] if len(steps) == 1 else stage.at[pl.ds(slot, len(steps))]
        writes.append(pltpu.make_async_copy(block, targets[index], out_sems.at[index]))
        slot += len(steps)
    for copies in reads:
        for copy in copies:
            copy.start()
    for copies, write in zip(reads, writes):
        for copy in copies:
            copy.wait()
        write.start()
    for write in writes:
        write.wait()


def split_heads(keys, values, layout, members):
    tokens, row_width = keys.shape
    piece = (2, tokens, row_width // members)
    shapes = [piece if len(steps) == 1 else (len(steps),) + piece for steps in layout]
    return pl.pallas_call(
        functools.partial(split_kernel, layout),
        in_specs=[HBM] * 2,
        out_specs=[ANY] * len(layout),
        out_shape=[jax.ShapeDtypeStruct(shape, keys.dtype) for shape in shapes],
        scratch_shapes=[
            pltpu.VMEM((members,) + piece, keys.dtype),
            pltpu.SemaphoreType.DMA((members, 2)),
            pltpu.SemaphoreType.DMA((len(layout),)),
        ],
        compiler_params=pltpu.CompilerParams(vmem_limit_bytes=SPLIT_VMEM),
        name="split_heads",
    )(keys, values)


def join_kernel(inner, *refs):
    count = len(inner)
    sources, target, sems = refs[:count], refs[count], refs[count + 1]
    width = sources[0].shape[-1]
    copies = []
    for step, (source, index) in enumerate(zip(sources, inner)):
        column = pl.multiple_of((own_index() ^ step) * width, width)
        source = source if index is None else source.at[index]
        copies.append(
            pltpu.make_async_copy(source, target.at[:, pl.ds(column, width)], sems.at[step])
        )
    for copy in copies:
        copy.start()
    for copy in copies:
        copy.wait()


def join_heads(pieces):
    arrays, inner = [piece[0] for piece in pieces], [piece[1] for piece in pieces]
    count = len(arrays)
    tokens, width = arrays[0].shape[-2:]
    return pl.pallas_call(
        functools.partial(join_kernel, inner),
        in_specs=[VMEM] * count,
        out_specs=HBM,
        out_shape=jax.ShapeDtypeStruct((tokens, count * width), arrays[0].dtype),
        scratch_shapes=[pltpu.SemaphoreType.DMA((count,))],
        compiler_params=pltpu.CompilerParams(vmem_limit_bytes=8 * 2**20),
        name="join_heads",
    )(*arrays)


def pack_kernel(first, second, target):
    target[0] = first[...]
    target[1] = second[...]


def pack(first, second):
    return pl.pallas_call(
        pack_kernel,
        in_specs=[VMEM] * 2,
        out_specs=VMEM,
        out_shape=jax.ShapeDtypeStruct((2,) + first.shape, first.dtype),
        compiler_params=pltpu.CompilerParams(vmem_limit_bytes=4 * 2**20),
        name="pack",
    )(first, second)


def assemble_kernel(places, members, head_size, *refs):
    arrays, targets = refs[:-2], refs[-2:]
    tokens = arrays[0].shape[-2]
    slab = head_size * tokens
    own = members * tokens
    for array, inner, step, halo in places:
        source = own_index() ^ step
        lane = (source % head_size) * tokens
        if halo:
            start = lane + jnp.where(source < head_size, slab + own, 0)
        else:
            start = slab + source * tokens
        rows = pl.ds(pl.multiple_of(start, 16), tokens)
        for part in range(2):
            ref = arrays[array]
            targets[part][rows] = ref[part] if inner is None else ref[inner, part]


def assemble(pieces, members, head_size):
    arrays = [piece[0] for piece in pieces]
    places = [(i, inner, step, halo) for i, (_, inner, step, halo) in enumerate(pieces)]
    tokens, width = arrays[0].shape[-2:]
    window = (members + 2 * head_size) * tokens
    return pl.pallas_call(
        functools.partial(assemble_kernel, places, members, head_size),
        in_specs=[VMEM] * len(arrays),
        out_specs=[VMEM] * 2,
        out_shape=[jax.ShapeDtypeStruct((window, width), arrays[0].dtype)] * 2,
        compiler_params=pltpu.CompilerParams(vmem_limit_bytes=24 * 2**20),
        name="assemble",
    )(*arrays)


def fold(value, op):
    parts = [value[i * 8 : (i + 1) * 8] for i in range(value.shape[0] // 8)]
    while len(parts) > 1:
        rest = [parts[-1]] if len(parts) % 2 else []
        parts = [op(a, b) for a, b in zip(parts[::2], parts[1::2])] + rest
    return parts[0]


def rows_of(tile):
    return pl.ds(pl.multiple_of(tile * TILE, TILE), TILE)


def attend_kernel(parts, pieces, inner, paired, *refs):
    outputs = len(parts) * pieces
    plan_in, q_refs = refs[: len(parts)], refs[len(parts) : len(parts) + outputs]
    keys, values = refs[len(parts) + outputs : len(parts) + outputs + 2]
    out_refs = refs[-11 - (outputs // 2 if paired else outputs) : -11]
    plans, sems, item_tile, item_slot, item_key, q_part, out_part, raw, peaks, acc, totals = refs[-11:]
    tokens = q_refs[0].shape[-2]
    block = pieces * tokens
    block_tiles = block // TILE
    tiles = len(parts) * block_tiles
    slab_tiles, slots = plan_in[0].shape[0], plan_in[0].shape[1] - 1
    copies = [
        pltpu.make_async_copy(plan, plans.at[i], sems.at[i]) for i, plan in enumerate(plan_in)
    ]
    for copy in copies:
        copy.start()
    me = own_index()
    base = (lax.axis_index("group") * lax.axis_size("member") - 1) * slab_tiles
    factor = HD**-0.5 * LOG2E

    def piece_rows(index, step):
        row = index * block + ((me % pieces) ^ step) * tokens
        return pl.ds(pl.multiple_of(row, 16), tokens)

    for index in range(len(parts)):
        for step in range(pieces):
            place = index * pieces + step
            ref = q_refs[place]
            q_part[piece_rows(index, step)] = (
                ref[...] if inner[place] is None else ref[inner[place]]
            )
    acc[...] = jnp.zeros_like(acc)
    totals[...] = jnp.zeros_like(totals)

    for copy in copies:
        copy.wait()
    total = jnp.int32(0)
    for index, part in enumerate(parts):
        first_row = (((me // pieces) ^ part) * block_tiles) % slab_tiles
        for tile in range(block_tiles):
            for slot in range(slots):
                item_tile[total + slot] = jnp.int32(index * block_tiles + tile)
                item_slot[total + slot] = jnp.int32(slot)
                item_key[total + slot] = plans[index, first_row + tile, slot] - base
            total = total + plans[index, first_row + tile, slots]
    for extra in range(UNROLL):
        item_tile[total + extra] = jnp.int32(tiles)
        item_slot[total + extra] = jnp.int32(0)
        item_key[total + extra] = jnp.int32(0)

    def score(item, buffer):
        tile = jnp.minimum(item_tile[item], tiles - 1)
        scores = lax.dot_general(
            keys[rows_of(item_key[item])],
            q_part[rows_of(tile)],
            (((1,), (1,)), ((), ())),
            preferred_element_type=jnp.float32,
        )
        raw[buffer] = scores
        peaks[buffer] = fold(scores, jnp.maximum)

    def gather(item, buffer, highest, sums):
        tile = item_tile[item]
        before = jnp.where(item_slot[item] == 0, -1e30, highest)
        highest = jnp.maximum(before, jnp.max(peaks[buffer], axis=0, keepdims=True))
        kept = jnp.exp2((before - highest) * factor)
        raised = jnp.exp2((raw[buffer] - highest) * factor)
        sums = sums * kept + jnp.sum(fold(raised, jnp.add), axis=0, keepdims=True)
        update = lax.dot_general(
            values[rows_of(item_key[item])],
            raised.astype(jnp.bfloat16),
            (((0,), (0,)), ((), ())),
            preferred_element_type=jnp.float32,
        )
        acc[tile] = acc[tile] * kept + update
        totals[tile] = sums
        return highest, sums

    score(0, 0)

    def chunk(size, start):
        def body(i, carry):
            for step in range(size):
                item = start + i * size + step
                score(item + 1, (step + 1) % 2)
                carry = gather(item, step % 2, *carry)
            return carry

        return body

    blank = jnp.zeros((1, TILE), jnp.float32)
    whole = total // UNROLL
    carry = lax.fori_loop(0, whole, chunk(UNROLL, 0), (blank, blank))
    rest = total - whole * UNROLL
    lax.fori_loop(0, (rest + 1) // 2, chunk(2, whole * UNROLL), carry)
    for tile in range(tiles):
        out_part[tile * TILE : (tile + 1) * TILE] = jnp.transpose(acc[tile] / totals[tile]).astype(
            out_part.dtype
        )
    for index in range(len(parts)):
        for step in range(pieces):
            place = index * pieces + step
            if paired:
                out_refs[place // 2][place % 2] = out_part[piece_rows(index, step)]
            else:
                out_refs[place][...] = out_part[piece_rows(index, step)]


def attend(plans, queries, keys, values, parts, pieces, paired):
    queries, inner = [q[0] for q in queries], [q[1] for q in queries]
    tokens, width = queries[0].shape[-2:]
    dtype = queries[0].dtype
    rows = len(parts) * pieces * tokens
    tiles = rows // TILE
    items = tiles * (plans[0].shape[1] - 1) + UNROLL + 8
    outputs = len(parts) * pieces
    return pl.pallas_call(
        functools.partial(attend_kernel, parts, pieces, inner, paired),
        in_specs=[VMEM] * (len(parts) + outputs + 2),
        out_specs=[VMEM] * (outputs // 2 if paired else outputs),
        out_shape=[jax.ShapeDtypeStruct((2, tokens, width), dtype)] * (outputs // 2)
        if paired
        else [jax.ShapeDtypeStruct((tokens, width), dtype)] * outputs,
        scratch_shapes=[
            pltpu.SMEM((len(parts),) + plans[0].shape, jnp.int32),
            pltpu.SemaphoreType.DMA((len(parts),)),
        ]
        + [pltpu.SMEM((items,), jnp.int32)] * 3
        + [pltpu.VMEM((rows, width), dtype)] * 2
        + [
            pltpu.VMEM((2, TILE, TILE), jnp.float32),
            pltpu.VMEM((2, 8, TILE), jnp.float32),
            pltpu.VMEM((tiles + 1, HD, TILE), jnp.float32),
            pltpu.VMEM((tiles + 1, 1, TILE), jnp.float32),
        ],
        compiler_params=pltpu.CompilerParams(vmem_limit_bytes=20 * 2**20),
        cost_estimate=pl.CostEstimate(
            flops=16 * rows * TILE * HD, bytes_accessed=4 * rows * width, transcendentals=0
        ),
        name="attend",
    )(*plans, *queries, keys, values)


def pieces_of(tokens):
    pieces = 1
    while pieces * tokens % TILE:
        pieces *= 2
    return pieces


def shards(group_size, queries, keys, values, tile_list, tile_count):
    groups = lax.axis_size("group")
    head_size = lax.axis_size("head")
    members = group_size * head_size
    tokens = queries.shape[0]
    pieces = pieces_of(tokens)

    def swap(piece, step):
        if step == 0:
            return piece
        pairs = [(g * members + i, g * members + (i ^ step)) for g in range(groups) for i in range(members)]
        return lax.ppermute(piece, AXES, pairs)

    def relay(piece, step):
        pairs = []
        for g in range(groups):
            for i in range(members):
                member = (i ^ step) // head_size
                if member == group_size - 1 and g + 1 < groups:
                    pairs.append((g * members + i, (g + 1) * members + i))
                if member == 0 and g > 0:
                    pairs.append((g * members + i, (g - 1) * members + i))
        return lax.ppermute(piece, AXES, pairs)

    own_plan = jnp.concatenate([tile_list, tile_count[:, None]], axis=1)
    plans = [swap(own_plan, step * head_size) for step in range(group_size)]

    layout = layout_of(members)
    kv_split = split_heads(keys, values, layout, members)
    swapped = {s: swap(array, s) for (s,), array in zip(layout, kv_split)}
    pieces_kv = [(array, None, step, False) for step, array in swapped.items()]
    for step in range(members // 4, members):
        beyond = relay(swapped[step], step)
        pieces_kv.append((beyond, None, step, True))
    for step in range(0, members // 4, 2):
        pair = pack(swapped[step], swapped[step + 1])
        beyond = relay(pair, step)
        pieces_kv += [(beyond, inner, step + inner, True) for inner in range(2)]

    quarter = members // 4
    paired_steps = [*range(0, quarter, 2), *range(3 * quarter, members, 2)]
    q_layout = [(s, s + 1) for s in paired_steps] + [(s,) for s in range(quarter, 3 * quarter)]
    q_pieces = {}
    for steps, piece in zip(q_layout, split_queries(queries, q_layout, members)):
        first = steps[0]
        piece = swap(piece, first)
        if len(steps) == 1:
            q_pieces[first] = (piece, None)
        else:
            q_pieces[first] = (piece, 0)
            q_pieces[first + 1] = (swap(piece, 1), 1)
    window_keys, window_values = assemble(pieces_kv, members, head_size)

    results = [None] * members
    for parts in calls_of(members // pieces):
        paired = parts[0] == members // pieces - 1
        steps = [part * pieces + step for part in parts for step in range(pieces)]
        outputs = attend(
            [plans[part * pieces // head_size] for part in parts],
            [q_pieces[step] for step in steps],
            window_keys,
            window_values,
            parts,
            pieces,
            paired,
        )
        if paired:
            for step, output in zip(steps[::2], outputs):
                output = swap(output, step)
                results[step] = (output, 0)
                results[step + 1] = (swap(output, 1), 1)
        else:
            for step, output in zip(steps, outputs):
                results[step] = (swap(output, step), None)
    return join_heads(results)


def calls_of(parts):
    return [(parts - 1,), tuple(range(parts - 2, 0, -1)), (0,)]


def layout_of(members):
    half = members // 2
    return [(s,) for s in [*range(members - 1, half - 1, -1), *range(half // 2, half), *range(half // 2)]]


def solution(mesh):
    tm_size, head_size = mesh.shape["tm"], mesh.shape["head"]

    def run(queries, keys, values, tile_list, tile_count):
        group_size = queries.shape[1] // HD // head_size
        members = group_size * head_size
        if group_size < 2 or members < 8 or tm_size % group_size or members & (members - 1):
            raise ValueError("unsupported mesh")
        fine = Mesh(mesh.devices.reshape(tm_size // group_size, group_size, head_size), AXES)
        tokens_spec = P(AXES, None)
        step = jax.shard_map(
            functools.partial(shards, group_size),
            mesh=fine,
            in_specs=(
                tokens_spec,
                tokens_spec,
                tokens_spec,
                P(("group", "member"), None),
                P(("group", "member")),
            ),
            out_specs=tokens_spec,
            check_vma=False,
        )
        return step(queries, keys, values, tile_list, tile_count)

    return run
```

```python
import functools

import jax
import jax.numpy as jnp
from jax import lax
from jax.experimental import pallas as pl
from jax.experimental.pallas import tpu as pltpu
from jax.sharding import Mesh, PartitionSpec as P


HD = 128
TILE = 384
UNROLL = 6
LOG2E = 1.4426950408889634
SPLIT_VMEM = 61 * 2**20
AXES = ("group", "member", "head")

ANY = pl.BlockSpec(memory_space=pl.ANY)
HBM = pl.BlockSpec(memory_space=pltpu.HBM)
SMEM = pl.BlockSpec(memory_space=pltpu.SMEM)
VMEM = pl.BlockSpec(memory_space=pltpu.VMEM)


def own_index():
    return lax.axis_index("member") * lax.axis_size("head") + lax.axis_index("head")


def split_kernel_q(layout, source, *refs):
    targets = refs[: len(layout)]
    stage, in_sems, out_sems = refs[len(layout) :]
    width = stage.shape[-1]

    def read(step):
        column = pl.multiple_of((own_index() ^ step) * width, width)
        return pltpu.make_async_copy(
            source.at[:, pl.ds(column, width)], stage.at[step], in_sems.at[step]
        )

    def write(index):
        first, size = layout[index][0], len(layout[index])
        block = stage.at[first] if size == 1 else stage.at[pl.ds(first, size)]
        return pltpu.make_async_copy(block, targets[index], out_sems.at[index])

    for steps in layout:
        for step in steps:
            read(step).start()
    for index, steps in enumerate(layout):
        for step in steps:
            read(step).wait()
        write(index).start()
    for index in range(len(layout)):
        write(index).wait()


def split_queries(source, layout, members):
    tokens, row_width = source.shape
    piece = (tokens, row_width // members)
    shapes = [piece if len(steps) == 1 else (len(steps),) + piece for steps in layout]
    return pl.pallas_call(
        functools.partial(split_kernel_q, layout),
        in_specs=[HBM],
        out_specs=[ANY] * len(layout),
        out_shape=[jax.ShapeDtypeStruct(shape, source.dtype) for shape in shapes],
        scratch_shapes=[
            pltpu.VMEM((members,) + piece, source.dtype),
            pltpu.SemaphoreType.DMA((members,)),
            pltpu.SemaphoreType.DMA((len(layout),)),
        ],
        compiler_params=pltpu.CompilerParams(vmem_limit_bytes=8 * 2**20),
        name="split_queries",
    )(source)


def split_kernel(layout, *refs):
    sources, targets = refs[:2], refs[2 : 2 + len(layout)]
    stage, in_sems, out_sems = refs[2 + len(layout) :]
    width = stage.shape[-1]

    def read(slot, step, array):
        column = pl.multiple_of((own_index() ^ step) * width, width)
        return pltpu.make_async_copy(
            sources[array].at[:, pl.ds(column, width)], stage.at[slot, array], in_sems.at[slot, array]
        )

    reads, writes, slot = [], [], 0
    for index, steps in enumerate(layout):
        reads.append([read(slot + k, s, array) for k, s in enumerate(steps) for array in range(2)])
        block = stage.at[slot] if len(steps) == 1 else stage.at[pl.ds(slot, len(steps))]
        writes.append(pltpu.make_async_copy(block, targets[index], out_sems.at[index]))
        slot += len(steps)
    for copies in reads:
        for copy in copies:
            copy.start()
    for copies, write in zip(reads, writes):
        for copy in copies:
            copy.wait()
        write.start()
    for write in writes:
        write.wait()


def split_heads(keys, values, layout, members):
    tokens, row_width = keys.shape
    piece = (2, tokens, row_width // members)
    shapes = [piece if len(steps) == 1 else (len(steps),) + piece for steps in layout]
    return pl.pallas_call(
        functools.partial(split_kernel, layout),
        in_specs=[HBM] * 2,
        out_specs=[ANY] * len(layout),
        out_shape=[jax.ShapeDtypeStruct(shape, keys.dtype) for shape in shapes],
        scratch_shapes=[
            pltpu.VMEM((members,) + piece, keys.dtype),
            pltpu.SemaphoreType.DMA((members, 2)),
            pltpu.SemaphoreType.DMA((len(layout),)),
        ],
        compiler_params=pltpu.CompilerParams(vmem_limit_bytes=SPLIT_VMEM),
        name="split_heads",
    )(keys, values)


def join_kernel(inner, *refs):
    count = len(inner)
    sources, target, sems = refs[:count], refs[count], refs[count + 1]
    width = sources[0].shape[-1]
    copies = []
    for step, (source, index) in enumerate(zip(sources, inner)):
        column = pl.multiple_of((own_index() ^ step) * width, width)
        source = source if index is None else source.at[index]
        copies.append(
            pltpu.make_async_copy(source, target.at[:, pl.ds(column, width)], sems.at[step])
        )
    for copy in copies:
        copy.start()
    for copy in copies:
        copy.wait()


def join_heads(pieces):
    arrays, inner = [piece[0] for piece in pieces], [piece[1] for piece in pieces]
    count = len(arrays)
    tokens, width = arrays[0].shape[-2:]
    return pl.pallas_call(
        functools.partial(join_kernel, inner),
        in_specs=[VMEM] * count,
        out_specs=HBM,
        out_shape=jax.ShapeDtypeStruct((tokens, count * width), arrays[0].dtype),
        scratch_shapes=[pltpu.SemaphoreType.DMA((count,))],
        compiler_params=pltpu.CompilerParams(vmem_limit_bytes=8 * 2**20),
        name="join_heads",
    )(*arrays)


def pack_kernel(first, second, target):
    target[0] = first[...]
    target[1] = second[...]


def pack(first, second):
    return pl.pallas_call(
        pack_kernel,
        in_specs=[VMEM] * 2,
        out_specs=VMEM,
        out_shape=jax.ShapeDtypeStruct((2,) + first.shape, first.dtype),
        compiler_params=pltpu.CompilerParams(vmem_limit_bytes=4 * 2**20),
        name="pack",
    )(first, second)


def assemble_kernel(places, members, head_size, *refs):
    arrays, targets = refs[:-2], refs[-2:]
    tokens = arrays[0].shape[-2]
    slab = head_size * tokens
    own = members * tokens
    for array, inner, step, halo in places:
        source = own_index() ^ step
        lane = (source % head_size) * tokens
        if halo:
            start = lane + jnp.where(source < head_size, slab + own, 0)
        else:
            start = slab + source * tokens
        rows = pl.ds(pl.multiple_of(start, 16), tokens)
        for part in range(2):
            ref = arrays[array]
            targets[part][rows] = ref[part] if inner is None else ref[inner, part]


def assemble(pieces, members, head_size):
    arrays = [piece[0] for piece in pieces]
    places = [(i, inner, step, halo) for i, (_, inner, step, halo) in enumerate(pieces)]
    tokens, width = arrays[0].shape[-2:]
    window = (members + 2 * head_size) * tokens
    return pl.pallas_call(
        functools.partial(assemble_kernel, places, members, head_size),
        in_specs=[VMEM] * len(arrays),
        out_specs=[VMEM] * 2,
        out_shape=[jax.ShapeDtypeStruct((window, width), arrays[0].dtype)] * 2,
        compiler_params=pltpu.CompilerParams(vmem_limit_bytes=24 * 2**20),
        name="assemble",
    )(*arrays)


def fold(value, op):
    parts = [value[i * 8 : (i + 1) * 8] for i in range(value.shape[0] // 8)]
    while len(parts) > 1:
        rest = [parts[-1]] if len(parts) % 2 else []
        parts = [op(a, b) for a, b in zip(parts[::2], parts[1::2])] + rest
    return parts[0]


def rows_of(tile):
    return pl.ds(pl.multiple_of(tile * TILE, TILE), TILE)


def attend_kernel(parts, pieces, inner, paired, *refs):
    outputs = len(parts) * pieces
    plan_in, q_refs = refs[: len(parts)], refs[len(parts) : len(parts) + outputs]
    keys, values = refs[len(parts) + outputs : len(parts) + outputs + 2]
    out_refs = list(refs[-11 - sum(pieces // 2 if p else pieces for p in paired) : -11])
    plans, sems, item_tile, item_slot, item_key, q_part, out_part, raw, peaks, acc, totals = refs[-11:]
    tokens = q_refs[0].shape[-2]
    block = pieces * tokens
    block_tiles = block // TILE
    tiles = len(parts) * block_tiles
    slab_tiles, slots = plan_in[0].shape[0], plan_in[0].shape[1] - 1
    copies = [
        pltpu.make_async_copy(plan, plans.at[i], sems.at[i]) for i, plan in enumerate(plan_in)
    ]
    for copy in copies:
        copy.start()
    me = own_index()
    base = (lax.axis_index("group") * lax.axis_size("member") - 1) * slab_tiles
    factor = HD**-0.5 * LOG2E

    def piece_rows(index, step):
        row = index * block + ((me % pieces) ^ step) * tokens
        return pl.ds(pl.multiple_of(row, 16), tokens)

    for index in range(len(parts)):
        for step in range(pieces):
            place = index * pieces + step
            ref = q_refs[place]
            q_part[piece_rows(index, step)] = (
                ref[...] if inner[place] is None else ref[inner[place]]
            )
    acc[...] = jnp.zeros_like(acc)
    totals[...] = jnp.zeros_like(totals)

    for copy in copies:
        copy.wait()
    total = jnp.int32(0)
    for index, part in enumerate(parts):
        first_row = (((me // pieces) ^ part) * block_tiles) % slab_tiles
        for tile in range(block_tiles):
            for slot in range(slots):
                item_tile[total + slot] = jnp.int32(index * block_tiles + tile)
                item_slot[total + slot] = jnp.int32(slot)
                item_key[total + slot] = plans[index, first_row + tile, slot] - base
            total = total + plans[index, first_row + tile, slots]
    for extra in range(UNROLL):
        item_tile[total + extra] = jnp.int32(tiles)
        item_slot[total + extra] = jnp.int32(0)
        item_key[total + extra] = jnp.int32(0)

    def score(item, buffer):
        tile = jnp.minimum(item_tile[item], tiles - 1)
        scores = lax.dot_general(
            keys[rows_of(item_key[item])],
            q_part[rows_of(tile)],
            (((1,), (1,)), ((), ())),
            preferred_element_type=jnp.float32,
        )
        raw[buffer] = scores
        peaks[buffer] = fold(scores, jnp.maximum)

    def gather(item, buffer, highest, sums):
        tile = item_tile[item]
        before = jnp.where(item_slot[item] == 0, -1e30, highest)
        highest = jnp.maximum(before, jnp.max(peaks[buffer], axis=0, keepdims=True))
        kept = jnp.exp2((before - highest) * factor)
        raised = jnp.exp2((raw[buffer] - highest) * factor)
        sums = sums * kept + jnp.sum(fold(raised, jnp.add), axis=0, keepdims=True)
        update = lax.dot_general(
            values[rows_of(item_key[item])],
            raised.astype(jnp.bfloat16),
            (((0,), (0,)), ((), ())),
            preferred_element_type=jnp.float32,
        )
        acc[tile] = acc[tile] * kept + update
        totals[tile] = sums
        return highest, sums

    score(0, 0)

    def chunk(size, start):
        def body(i, carry):
            for step in range(size):
                item = start + i * size + step
                score(item + 1, (step + 1) % 2)
                carry = gather(item, step % 2, *carry)
            return carry

        return body

    blank = jnp.zeros((1, TILE), jnp.float32)
    whole = total // UNROLL
    carry = lax.fori_loop(0, whole, chunk(UNROLL, 0), (blank, blank))
    rest = total - whole * UNROLL
    lax.fori_loop(0, (rest + 1) // 2, chunk(2, whole * UNROLL), carry)
    for tile in range(tiles):
        out_part[tile * TILE : (tile + 1) * TILE] = jnp.transpose(acc[tile] / totals[tile]).astype(
            out_part.dtype
        )
    for index in range(len(parts)):
        for step in range(pieces):
            value = out_part[piece_rows(index, step)]
            if not paired[index]:
                out_refs.pop(0)[...] = value
            elif step % 2 == 0:
                out_refs[0][0] = value
            else:
                out_refs.pop(0)[1] = value


def attend(plans, queries, keys, values, parts, pieces, paired):
    queries, inner = [q[0] for q in queries], [q[1] for q in queries]
    tokens, width = queries[0].shape[-2:]
    dtype = queries[0].dtype
    rows = len(parts) * pieces * tokens
    tiles = rows // TILE
    items = tiles * (plans[0].shape[1] - 1) + UNROLL + 8
    outputs = len(parts) * pieces
    shapes = []
    for pair in paired:
        shapes += [(2, tokens, width)] * (pieces // 2) if pair else [(tokens, width)] * pieces
    return pl.pallas_call(
        functools.partial(attend_kernel, parts, pieces, inner, paired),
        in_specs=[VMEM] * (len(parts) + outputs + 2),
        out_specs=[VMEM] * len(shapes),
        out_shape=[jax.ShapeDtypeStruct(shape, dtype) for shape in shapes],
        scratch_shapes=[
            pltpu.SMEM((len(parts),) + plans[0].shape, jnp.int32),
            pltpu.SemaphoreType.DMA((len(parts),)),
        ]
        + [pltpu.SMEM((items,), jnp.int32)] * 3
        + [pltpu.VMEM((rows, width), dtype)] * 2
        + [
            pltpu.VMEM((2, TILE, TILE), jnp.float32),
            pltpu.VMEM((2, 8, TILE), jnp.float32),
            pltpu.VMEM((tiles + 1, HD, TILE), jnp.float32),
            pltpu.VMEM((tiles + 1, 1, TILE), jnp.float32),
        ],
        compiler_params=pltpu.CompilerParams(vmem_limit_bytes=20 * 2**20),
        cost_estimate=pl.CostEstimate(
            flops=16 * rows * TILE * HD, bytes_accessed=4 * rows * width, transcendentals=0
        ),
        name="attend",
    )(*plans, *queries, keys, values)


def pieces_of(tokens):
    pieces = 1
    while pieces * tokens % TILE:
        pieces *= 2
    return pieces


def shards(group_size, queries, keys, values, tile_list, tile_count):
    groups = lax.axis_size("group")
    head_size = lax.axis_size("head")
    members = group_size * head_size
    tokens = queries.shape[0]
    pieces = pieces_of(tokens)

    def swap(piece, step):
        if step == 0:
            return piece
        pairs = [(g * members + i, g * members + (i ^ step)) for g in range(groups) for i in range(members)]
        return lax.ppermute(piece, AXES, pairs)

    def relay(piece, step):
        pairs = []
        for g in range(groups):
            for i in range(members):
                member = (i ^ step) // head_size
                if member == group_size - 1 and g + 1 < groups:
                    pairs.append((g * members + i, (g + 1) * members + i))
                if member == 0 and g > 0:
                    pairs.append((g * members + i, (g - 1) * members + i))
        return lax.ppermute(piece, AXES, pairs)

    own_plan = jnp.concatenate([tile_list, tile_count[:, None]], axis=1)
    plans = [swap(own_plan, step * head_size) for step in range(group_size)]

    layout = layout_of(members)
    kv_split = split_heads(keys, values, layout, members)
    swapped = {s: swap(array, s) for (s,), array in zip(layout, kv_split)}
    pieces_kv = [(array, None, step, False) for step, array in swapped.items()]
    for step in range(members // 4, members):
        beyond = relay(swapped[step], step)
        pieces_kv.append((beyond, None, step, True))
    for step in range(0, members // 4, 2):
        pair = pack(swapped[step], swapped[step + 1])
        beyond = relay(pair, step)
        pieces_kv += [(beyond, inner, step + inner, True) for inner in range(2)]

    quarter = members // 4
    paired_steps = [*range(0, quarter, 2), *range(3 * quarter, members, 2)]
    q_layout = [(s, s + 1) for s in paired_steps] + [(s,) for s in range(quarter, 3 * quarter)]
    q_pieces = {}
    for steps, piece in zip(q_layout, split_queries(queries, q_layout, members)):
        first = steps[0]
        piece = swap(piece, first)
        if len(steps) == 1:
            q_pieces[first] = (piece, None)
        else:
            q_pieces[first] = (piece, 0)
            q_pieces[first + 1] = (swap(piece, 1), 1)
    window_keys, window_values = assemble(pieces_kv, members, head_size)

    results = [None] * members
    for parts in calls_of(members // pieces):
        paired = [part >= members // pieces // 2 for part in parts]
        steps = [part * pieces + step for part in parts for step in range(pieces)]
        outputs = attend(
            [plans[part * pieces // head_size] for part in parts],
            [q_pieces[step] for step in steps],
            window_keys,
            window_values,
            parts,
            pieces,
            paired,
        )
        outputs = list(outputs)
        for step in steps:
            if not paired[parts.index(step // pieces)]:
                results[step] = (swap(outputs.pop(0), step), None)
            elif step % 2 == 0:
                output = swap(outputs.pop(0), step)
                results[step] = (output, 0)
                results[step + 1] = (swap(output, 1), 1)
    return join_heads(results)


def calls_of(parts):
    return [(parts - 1,), tuple(range(parts - 2, 0, -1)), (0,)]


def layout_of(members):
    half = members // 2
    return [(s,) for s in [*range(members - 1, half - 1, -1), *range(half // 2, half), *range(half // 2)]]


def solution(mesh):
    tm_size, head_size = mesh.shape["tm"], mesh.shape["head"]

    def run(queries, keys, values, tile_list, tile_count):
        group_size = queries.shape[1] // HD // head_size
        members = group_size * head_size
        if group_size < 2 or members < 8 or tm_size % group_size or members & (members - 1):
            raise ValueError("unsupported mesh")
        fine = Mesh(mesh.devices.reshape(tm_size // group_size, group_size, head_size), AXES)
        tokens_spec = P(AXES, None)
        step = jax.shard_map(
            functools.partial(shards, group_size),
            mesh=fine,
            in_specs=(
                tokens_spec,
                tokens_spec,
                tokens_spec,
                P(("group", "member"), None),
                P(("group", "member")),
            ),
            out_specs=tokens_spec,
            check_vma=False,
        )
        return step(queries, keys, values, tile_list, tile_count)

    return run
```
